128 devices in a mesh: row: 8 (over x, core), col: 16 (over z, y).
Axes of the slice: x: 4, y: 4, z: 4, core: 2. Of those that a mesh axis runs over, the one named last changes fastest.
Arguments:
- kernel: bfloat16 [32768, 32768], P('row', 'col'), may hold values from -1 to 1
- random_cols: bfloat16 [32768, 256], P('row'), may hold values from -6 to 6
- tree_perm: int32 [32768], replicated, may hold values from 0 to 32767, as said below
- leaf_units: int32 [32], replicated, may hold values from 1 to 8, 160 in all
Outputs:
- bases: bfloat16 [4, 32768, 256], P(None, ('row', 'col'))
The draws below stay inside these ranges and needn't reach their ends.
Inputs may be any that keep to these rules, and one draw needn't show every extreme that they name: `tree_perm`: A permutation. Cut tree positions and stored rows alike into blocks of 256 in order: every tree block takes at most 2 rows from any one stored block, some pair of blocks shares exactly 2, and every stored block gives 256 rows in all. `leaf_units`: they sum to 160.
All inputs are finite; a program needn't handle non-finite values.
Results may differ from the reference program's by a relative error of at most 0.0067.
Values may be sent and summed in bfloat16 or wider, within the bound.
No kernel may reach another device: no remote copies, remote signals or barrier semaphores. Data moves between devices by JAX's collectives and lax.ppermute only.
A program may use at most 192 MiB of HBM per device.

```python
import math
import jax
import jax.numpy as jnp
import numpy as np
from jax import lax

N = 32768
S = 256
UNIT = 128
MINU = 4
MOSTU = 8
LEAVES = 32
LEVELS = 3
ROWS_DEV = 256


def draw_kernel(key, part):
    point_key, noise_key, weight_key = jax.random.split(key, 3)
    spread_width = 0.08
    amplitude = 0.5
    points = jax.random.uniform(point_key, (N, 3), jnp.float32)
    norms = jnp.sum(points * points, axis=1)
    block = min(N, 512)
    groups = N // ROWS_DEV
    spacing = jax.random.permutation(weight_key, groups).astype(jnp.float32) / max(groups - 1, 1)
    group_weight = jnp.exp(jnp.log(10.0) * spacing)
    row_weight = jnp.repeat(group_weight, ROWS_DEV, total_repeat_length=N)

    def one_block(index):
        chosen = lax.dynamic_slice_in_dim(points, index * block, block, 0)
        chosen_norms = lax.dynamic_slice_in_dim(norms, index * block, block, 0)
        chosen_weight = lax.dynamic_slice_in_dim(row_weight, index * block, block, 0)
        cross = jnp.dot(chosen, points.T, precision=lax.Precision.HIGHEST)
        distance = jnp.maximum(chosen_norms[:, None] + norms[None, :] - 2.0 * cross, 0.0)
        noise = jax.random.truncated_normal(jax.random.fold_in(noise_key, index), -4.0, 4.0, (block, N), jnp.float32)
        entries = (jnp.exp(-distance / (2.0 * spread_width * spread_width)) + amplitude * noise) * N ** (-0.5)
        return (entries * chosen_weight[:, None]).astype(jnp.bfloat16)
    blocks = lax.map(one_block, jnp.arange(N // block, dtype=jnp.int32))
    return blocks.reshape(N, N)


def random_rows(key, count, length):
    scores = jax.random.randint(key, (count, length), 0, 2 ** 20) * length + jnp.arange(length, dtype=jnp.int32)[None, :]
    return jnp.argsort(scores, axis=1).astype(jnp.int32)


def draw_tree_perm(key, part):
    devices = N // ROWS_DEV
    first_key, second_key, third_key = jax.random.split(jax.random.fold_in(key, 17), 3)
    device_order = jax.random.permutation(first_key, devices).astype(jnp.int32)
    within = random_rows(second_key, devices, ROWS_DEV)
    base = (jnp.arange(devices, dtype=jnp.int32) * ROWS_DEV)[:, None]
    source = jnp.take(device_order, (within + base) % devices).reshape(-1)
    grouped = jnp.argsort(source * N + jnp.arange(N, dtype=jnp.int32)).astype(jnp.int32)
    ranks = random_rows(third_key, devices, ROWS_DEV)
    stored = (base + ranks).reshape(-1)
    return jnp.zeros((N,), jnp.int32).at[grouped].set(stored)


def levels(stream_key, dims, cuts, smallest, largest):
    level = 1.0
    for position, blocks in cuts:
        steps = jax.random.uniform(jax.random.fold_in(jax.random.fold_in(stream_key, 6), position), (blocks,), jnp.float32, smallest / len(cuts), largest / len(cuts))
        level = level * jnp.repeat(jnp.exp(steps), dims[position] // blocks).reshape((-1,) + (1,) * (len(dims) - 1 - position))
    return level


def profile(count, total, bound, lean):
    loads = [(1 << 20) // math.isqrt(standing ** lean) + 1 for standing in range(2, count + 1)]
    surplus, counts = total - bound - (count - 1), [1] * (count - 1)
    while surplus > 0:
        candidates = [i for i in range(count - 1) if counts[i] < bound]
        whole, left = sum([loads[i] for i in candidates]), surplus
        for i in candidates:
            extra = min(bound - counts[i], max(1, left * loads[i] // whole), surplus)
            counts[i] = counts[i] + extra
            surplus = surplus - extra
    return np.array([bound] + counts)


def uneven(rng, number_of, total, most, skew):
    if number_of == 2:
        one = jax.random.randint(rng, (), max(1, total - most), min(most, total - 1) + 1)
        return jnp.stack([one, total - one])
    lengths = jnp.asarray(profile(number_of, total, most, skew), jnp.int32)
    twos = (number_of - 1) // 2
    giver, taker = lengths[1:1 + 2 * twos:2], lengths[2:2 + 2 * twos:2]
    room = jnp.minimum(giver - 1, most - taker)
    moved = jax.random.randint(jax.random.fold_in(rng, 1), (twos,), 0, 1 << 20) % (room + 1)
    lengths = lengths.at[1:1 + 2 * twos:2].set(giver - moved).at[2:2 + 2 * twos:2].set(taker + moved)
    return lengths[jax.random.permutation(jax.random.fold_in(rng, 2), number_of)]


def centred(rng, shape, deviation, reach, cuts=(), kind=jnp.bfloat16):
    factor_of = levels(rng, shape, cuts, -0.22, 0.18) if cuts else 1.0
    drawn = jax.random.normal(rng, shape, jnp.float32) * deviation * factor_of
    return jnp.minimum(jnp.maximum(drawn, -reach), reach).astype(kind)


def setup_inputs(seed: int = 0) -> dict:
    key_list = jax.random.split(jax.random.key(seed), 5)
    return {
        "kernel": draw_kernel(jax.random.fold_in(key_list[4], 71), 0),
        "random_cols": centred(key_list[1], (N, S), 1.0, 6.0, ((0, 8),)),
        "tree_perm": draw_tree_perm(jax.random.fold_in(key_list[4], 71), 0),
        "leaf_units": uneven(key_list[3], LEAVES, N // UNIT - (MINU - 1) * LEAVES, MOSTU, 1).astype(jnp.int32),
    }


def reference(kernel, random_cols, tree_perm, leaf_units):
    partial_w = lax.dot_general(kernel.astype(jnp.float32), random_cols.astype(jnp.float32), (((0,), (0,)), ((), ())), preferred_element_type=jnp.float32)
    sample_w = partial_w.astype(jnp.bfloat16)
    sample = jnp.dot(kernel.astype(jnp.float32), sample_w.astype(jnp.float32), preferred_element_type=jnp.float32).astype(jnp.bfloat16)
    tree_rows = jnp.take(sample, tree_perm.astype(jnp.int32), axis=0)
    sizes = (UNIT * (MINU - 1 + leaf_units)).astype(jnp.int32)
    ends = jnp.cumsum(sizes).astype(jnp.int32)
    positions = jnp.arange(N, dtype=jnp.int32)
    leaf_of = jnp.sum(positions[:, None] >= ends[None, :], axis=1).astype(jnp.int32)

    def leaf_gram(leaf):
        masked = jnp.where((leaf_of == leaf)[:, None], tree_rows, jnp.zeros((), jnp.bfloat16))
        return jnp.dot(masked.T.astype(jnp.float32), tree_rows.astype(jnp.float32), preferred_element_type=jnp.float32)
    leaf_grams = lax.map(leaf_gram, jnp.arange(LEAVES, dtype=jnp.int32))
    values = tree_rows.astype(jnp.float32)
    results = []
    for level in range(LEVELS + 1):
        group = 2 ** level
        count = LEAVES // group
        node_grams = leaf_grams.reshape(count, group, S, S).sum(axis=1)
        node_sizes = sizes.reshape(count, group).sum(axis=1).astype(jnp.float32)
        factor = jnp.linalg.cholesky(node_grams / node_sizes[:, None, None])
        node_of = leaf_of // group

        def add_node(total, node):
            solved = jax.scipy.linalg.solve_triangular(factor[node], values.T, lower=True).T
            return (total + jnp.where((node_of == node)[:, None], solved, jnp.zeros((), jnp.float32)), None)
        total, unused = lax.scan(add_node, jnp.zeros((N, S), jnp.float32), jnp.arange(count, dtype=jnp.int32))
        results.append(total.astype(jnp.bfloat16))
    return jnp.stack(results)
```

```python
import functools

import jax
import jax.numpy as jnp
from jax import lax
from jax.experimental import pallas as pl
from jax.experimental.pallas import tpu as pltpu
from jax.sharding import PartitionSpec as P

UNIT = 128
MINU = 4
LEVELS = 3
BOTH = ("row", "col")
HIGHEST = lax.Precision.HIGHEST


def iota(shape, dim):
    return lax.broadcasted_iota(jnp.int32, shape, dim)


def second_pass(first_ref, kernel_ref, w_ref, tree_ref, out_ref, spread_ref):
    step = pl.program_id(0)
    panel = pl.num_programs(0)
    partial = jnp.dot(
        kernel_ref[...], w_ref[...], preferred_element_type=jnp.float32
    ).astype(jnp.bfloat16)
    tree = tree_ref[...]
    blocks, rows = tree.shape
    here = lax.shift_right_logical(tree, 8) == first_ref[0] + step
    inner = lax.bitwise_and(tree, rows - 1)
    low = jnp.min(jnp.where(here, inner, rows), axis=1, keepdims=True)
    high = jnp.max(jnp.where(here, inner, -1), axis=1, keepdims=True)
    lanes = iota((blocks, rows), 1)
    for which, chosen in enumerate((low, high)):
        pick = (lanes == chosen).astype(jnp.float32).astype(jnp.bfloat16)
        moved = jnp.dot(pick, partial, preferred_element_type=jnp.float32)
        width = moved.shape[1]
        for half in range(width // 128):
            column = which * (width // 128) + half
            spread_ref[column, pl.ds(step, blocks, stride=panel), :] = moved[
                :, half * 128 : (half + 1) * 128
            ]

    @pl.when(step == panel - 1)
    def _():
        for column in range(spread_ref.shape[0]):
            out_ref[:, column * 128 : (column + 1) * 128] = spread_ref[column].astype(
                jnp.bfloat16
            )


def collect(wanted_ref, parts_ref, rows_ref, gram_ref):
    row_devices, col_devices, inner, wide = parts_ref.shape
    blocks = row_devices * inner
    width = wide // 2
    groups = []
    for row in range(row_devices):
        total = parts_ref[row, 0].astype(jnp.float32)
        for col in range(1, col_devices):
            total = total + parts_ref[row, col].astype(jnp.float32)
        groups.append(total.astype(jnp.bfloat16))
    sample = jnp.concatenate(groups, axis=0)
    wanted = wanted_ref[...]
    rows = wanted.shape[0]
    block = lax.shift_right_logical(wanted, 8)
    inside = lax.bitwise_and(wanted, rows - 1)
    same = block == iota((rows, blocks), 1)
    low = jnp.min(jnp.where(same, inside, rows), axis=0, keepdims=True)
    high = jnp.max(jnp.where(same, inside, -1), axis=0, keepdims=True)
    ordered = jnp.zeros((rows, width), jnp.float32)
    for which, chosen in enumerate((low, high)):
        pick = jnp.where(same & (inside == chosen), 1.0, 0.0).astype(jnp.bfloat16)
        ordered = ordered + jnp.dot(
            pick,
            sample[:, which * width : (which + 1) * width],
            preferred_element_type=jnp.float32,
        )
    ordered = ordered.astype(jnp.bfloat16)
    rows_ref[...] = ordered
    half = width // 2
    for unit in range(rows // UNIT):
        piece = ordered[unit * UNIT : (unit + 1) * UNIT]
        left, right = piece[:, :half], piece[:, half:]
        pairs = ((left, left), (right, left), (right, right))
        for index, (one, two) in enumerate(pairs):
            gram = lax.dot_general(
                one, two, (((0,), (0,)), ((), ())), preferred_element_type=jnp.float32
            )
            gram_ref[pl.ds(unit * 4 + index, half, stride=8), :] = gram
        gram_ref[pl.ds(unit * 4 + 3, half, stride=8), :] = jnp.zeros(
            (half, half), jnp.float32
        )


def leaf_of_unit(units_ref, unit):
    leaf = jnp.zeros_like(unit)
    end = jnp.int32(0)
    for index in range(units_ref.shape[0]):
        end = end + units_ref[index] + (MINU - 1)
        leaf = leaf + (unit >= end).astype(jnp.int32)
    return leaf


def node_sums(units_ref, parts_ref, out_ref):
    devices = out_ref.shape[0]
    units = 2 * devices
    slots = 2 * (LEVELS + 1)
    unit_leaf = leaf_of_unit(units_ref, iota((8, units), 1))[0:1]
    row = iota((devices * slots, 128), 0)
    slot = lax.bitwise_and(row, slots - 1)
    level = lax.shift_right_logical(slot, 1)
    own = 2 * lax.shift_right_logical(row, 3) + lax.bitwise_and(slot, 1)
    own_node = lax.shift_right_logical(leaf_of_unit(units_ref, own), level)
    member = []
    for part in range(units // 128):
        leaf = jnp.broadcast_to(unit_leaf[:, part * 128 : (part + 1) * 128], row.shape)
        match = lax.shift_right_logical(leaf, level) == own_node
        member.append(jnp.where(match, 1.0, 0.0).astype(jnp.bfloat16))
    member = jnp.concatenate(member, axis=1)
    for index in range(3):
        left = parts_ref[pl.ds(index, units, stride=4), :]
        total = jnp.zeros((devices * slots, left.shape[1]), jnp.float32)
        for _ in range(3):
            piece = left.astype(jnp.bfloat16)
            left = left - piece.astype(jnp.float32)
            total = total + jnp.dot(member, piece, preferred_element_type=jnp.float32)
        out_ref[:, index * slots : (index + 1) * slots, :] = total.reshape(
            devices, slots, total.shape[1]
        )


def spread_lane(values, lane):
    return jnp.take_along_axis(values, jnp.full(values.shape, lane, jnp.int32), axis=1)


def invert_factors(work_ref, solved_ref):
    count, size, lanes = work_ref.shape
    lane = iota((8, lanes), 1)
    sub = iota((8, lanes), 0)
    chunk = 4

    def block_step(block, carry):
        base = pl.multiple_of(block * 8, 8)
        inside = (lane >= base) & (lane < base + 8)
        eye = lane - base == sub
        for which in range(count):
            rows = work_ref[which, pl.ds(base, 8), :]
            columns = [spread_lane(rows, base + i) for i in range(8)]
            value = jnp.where(inside, jnp.where(eye, 1.0, 0.0), rows)
            scales = []
            for i in range(8):
                pivot = jnp.broadcast_to(columns[i][i : i + 1], sub.shape)
                scale = lax.rsqrt(pivot)
                scales.append(scale)
                below = jnp.where(sub > i, columns[i] * scale, 0.0)
                keep = jnp.where(sub == i, scale, 1.0)
                for k in range(i, 8):
                    top = jnp.broadcast_to(columns[k][i : i + 1], sub.shape) * scale
                    columns[k] = columns[k] * keep - below * top
                top = jnp.broadcast_to(value[i : i + 1], sub.shape) * scale
                value = value * keep - below * top
            work_ref[which, pl.ds(base, 8), :] = jnp.where(lane <= base + sub, value, 0.0)
            for i in reversed(range(8)):
                top = jnp.broadcast_to(value[i : i + 1], sub.shape) * scales[i]
                above = jnp.where(sub < i, columns[i], 0.0)
                value = jnp.where(sub == i, top, value) - above * top
            solved_ref[which] = value

        def update(group, carry):
            for inner in range(chunk):
                index = group * chunk + inner
                start = pl.multiple_of(index * 8, 8)
                later = jnp.full(sub.shape, index, jnp.int32) > block
                for which in range(count):
                    rows = work_ref[which, pl.ds(start, 8), :]
                    total = jnp.where(inside, 0.0, rows)
                    for i in range(8):
                        row = jnp.broadcast_to(solved_ref[which, i : i + 1, :], sub.shape)
                        total = total - spread_lane(rows, base + i) * row
                    work_ref[which, pl.ds(start, 8), :] = jnp.where(later, total, rows)
            return carry

        return lax.fori_loop((block + 1) // chunk, size // 8 // chunk, update, carry)

    lax.fori_loop(0, size // 8, block_step, 0)


def dot_t(one, two, precision=HIGHEST):
    return lax.dot_general(
        one,
        two,
        (((1,), (1,)), ((), ())),
        precision=precision,
        preferred_element_type=jnp.float32,
    )


def node_bases(
    device_ref, units_ref, node_ref, rows_ref, out_ref, work_ref, side_ref, last_ref, solved_ref
):
    slots = work_ref.shape[0]
    half = work_ref.shape[1]
    stride = 3 * slots
    scales = []
    for slot in range(slots):
        level, unit = slot // 2, 2 * device_ref[0] + slot % 2
        leaf = jnp.int32(0)
        end = jnp.int32(0)
        for index in range(units_ref.shape[0]):
            end = end + units_ref[index] + (MINU - 1)
            leaf = leaf + (unit >= end).astype(jnp.int32)
        node = lax.shift_right_logical(leaf, level)
        count = jnp.int32(0)
        for index in range(units_ref.shape[0]):
            size = units_ref[index] + (MINU - 1)
            count = count + jnp.where(node == index >> level, size, 0)
        size = jnp.full((half, half), count * UNIT, jnp.int32).astype(jnp.float32)
        scales.append(size)
    for slot in range(slots):
        work_ref[slot] = node_ref[pl.ds(slot, half, stride=stride), :] / scales[slot]
    invert_factors(work_ref, solved_ref)
    for slot in range(slots):
        below = node_ref[pl.ds(slots + slot, half, stride=stride), :] / scales[slot]
        side = dot_t(below, work_ref[slot])
        side_ref[slot] = side
        corner = node_ref[pl.ds(2 * slots + slot, half, stride=stride), :] / scales[slot]
        last_ref[slot] = corner - dot_t(side, side)
    invert_factors(last_ref, solved_ref)
    for slot in range(slots):
        level, unit = slot // 2, slot % 2
        piece = rows_ref[unit * UNIT : (unit + 1) * UNIT, :].astype(jnp.float32)
        first = dot_t(piece[:, :half], work_ref[slot])
        rest = piece[:, half:] - dot_t(first, side_ref[slot])
        second = dot_t(rest, last_ref[slot])
        place = slice(unit * UNIT, (unit + 1) * UNIT)
        out_ref[level, place, :half] = first.astype(jnp.bfloat16)
        out_ref[level, place, half:] = second.astype(jnp.bfloat16)


def shards(kernel, random_cols, tree_perm, leaf_units):
    f32, bf16 = jnp.float32, jnp.bfloat16
    width = random_cols.shape[1]
    half = width // 2
    row_devices, col_devices = lax.axis_size("row"), lax.axis_size("col")
    devices = row_devices * col_devices
    total_rows = tree_perm.shape[0]
    rows_dev = total_rows // devices
    panel = kernel.shape[0] // rows_dev
    slots = 2 * (LEVELS + 1)
    row = lax.axis_index("row")
    device = row * col_devices + lax.axis_index("col")
    vmem = pl.BlockSpec(memory_space=pltpu.VMEM)
    smem = pl.BlockSpec(memory_space=pltpu.SMEM)

    def exchange(values, axes):
        return lax.all_to_all(values, axes, 0, 0, tiled=True)

    partial_w = lax.dot_general(
        kernel, random_cols, (((0,), (0,)), ((), ())), preferred_element_type=f32
    ).astype(bf16)
    chunk = kernel.shape[1] // row_devices
    arrived = exchange(partial_w.reshape(row_devices, chunk, width), "row")
    own_w = jnp.sum(arrived.astype(f32), axis=0).astype(bf16)
    sample_w = exchange(jnp.broadcast_to(own_w[None], (row_devices, chunk, width)), "row")
    sample_w = sample_w.reshape(kernel.shape[1], width)

    tree = tree_perm.reshape(devices, rows_dev)
    parts = pl.pallas_call(
        second_pass,
        grid_spec=pltpu.PrefetchScalarGridSpec(
            num_scalar_prefetch=1,
            grid=(panel,),
            in_specs=[
                pl.BlockSpec((rows_dev, kernel.shape[1]), lambda s, first: (s, 0)),
                pl.BlockSpec((kernel.shape[1], width), lambda s, first: (0, 0)),
                pl.BlockSpec((devices, rows_dev), lambda s, first: (0, 0)),
            ],
            out_specs=pl.BlockSpec((devices * panel, 2 * width), lambda s, first: (0, 0)),
            scratch_shapes=[pltpu.VMEM((4, devices * panel, 128), f32)],
        ),
        out_shape=jax.ShapeDtypeStruct((devices * panel, 2 * width), bf16),
        name="second_pass",
    )((row * panel)[None], kernel, sample_w, tree)
    parts = exchange(parts.reshape(devices, panel, 2 * width), BOTH)

    wanted = lax.dynamic_slice_in_dim(tree_perm, device * rows_dev, rows_dev)
    wanted = jnp.broadcast_to(wanted[:, None], (rows_dev, devices))
    tree_rows, grams = pl.pallas_call(
        collect,
        in_specs=[vmem, vmem],
        out_specs=[vmem, vmem],
        out_shape=[
            jax.ShapeDtypeStruct((rows_dev, width), bf16),
            jax.ShapeDtypeStruct((devices * 8, half), f32),
        ],
        name="collect",
    )(wanted, parts.reshape(row_devices, col_devices, panel, 2 * width))

    grams = exchange(grams.reshape(devices, 8, half), BOTH)
    nodes = pl.pallas_call(
        node_sums,
        in_specs=[smem, vmem],
        out_specs=vmem,
        out_shape=jax.ShapeDtypeStruct((devices, 3 * slots, half), f32),
        name="node_sums",
    )(leaf_units, grams.reshape(devices * 8, half))
    nodes = exchange(nodes, BOTH)

    return pl.pallas_call(
        node_bases,
        in_specs=[smem, smem, vmem, vmem],
        out_specs=vmem,
        out_shape=jax.ShapeDtypeStruct((LEVELS + 1, rows_dev, width), bf16),
        scratch_shapes=[pltpu.VMEM((slots, half, half), f32)] * 3
        + [pltpu.VMEM((slots, 8, half), f32)],
        name="node_bases",
    )(device[None], leaf_units, nodes.reshape(devices * 3 * slots, half), tree_rows)


def solution(mesh):
    return jax.shard_map(
        shards,
        mesh=mesh,
        in_specs=(P("row", "col"), P("row", None), P(), P()),
        out_specs=P(None, ("row", "col"), None),
        check_vma=False,
    )
```

```python
import functools

import jax
import jax.numpy as jnp
from jax import lax
from jax.experimental import pallas as pl
from jax.experimental.pallas import tpu as pltpu
from jax.sharding import PartitionSpec as P

UNIT = 128
MINU = 4
LEVELS = 3
DEEP = 32
TOGETHER = 4
EACH = 2
BOTH = ("row", "col")
HIGHEST = lax.Precision.HIGHEST


def iota(shape, dim):
    return lax.broadcasted_iota(jnp.int32, shape, dim)


def choose(first_ref, tree_ref, out_ref, turned_ref):
    panel = out_ref.shape[0]
    rows, blocks = turned_ref.shape[1:]
    tree = jnp.transpose(tree_ref[...])
    turned_ref[0] = lax.shift_right_logical(tree, 8)
    turned_ref[1] = lax.bitwise_and(tree, rows - 1)
    place = iota((rows, blocks), 0)

    def one(step, carry):
        here = turned_ref[0] == first_ref[0] + step
        inner = turned_ref[1]
        low = jnp.min(jnp.where(here, inner, rows), axis=0, keepdims=True)
        high = jnp.max(jnp.where(here, inner, -1), axis=0, keepdims=True)
        for which, chosen in enumerate((low, high)):
            pick = jnp.transpose(jnp.where(place == chosen, 1.0, 0.0))
            out_ref[step, which * blocks : (which + 1) * blocks, :] = pick.astype(jnp.bfloat16)
        return carry

    lax.fori_loop(0, panel, one, 0)


def second_pass(kernel_ref, w_ref, pick_ref, out_ref, held_ref, ready_ref, spread_ref, sems):
    panel, blocks = pick_ref.shape[0], pick_ref.shape[1] // 2
    steps, tall, _ = held_ref.shape
    rows = pick_ref.shape[2]
    each = tall // rows

    def fetch(index):
        return pltpu.make_async_copy(
            kernel_ref.at[pl.ds(index * tall, tall), :], held_ref.at[index], sems.at[index]
        )

    def product(index):
        return jnp.dot(
            held_ref[index], w_ref[...], preferred_element_type=jnp.float32
        ).astype(jnp.bfloat16)

    def move(index):
        for inner in range(each):
            moved = jnp.dot(
                pick_ref[index * each + inner],
                ready_ref[inner * rows : (inner + 1) * rows, :],
                preferred_element_type=jnp.float32,
            )
            for column in range(spread_ref.shape[0]):
                which, half = column // 2, column % 2
                place = pl.ds(index * each + inner, blocks, stride=panel + 1)
                spread_ref[column, place, :] = moved[
                    which * blocks : (which + 1) * blocks, half * 128 : (half + 1) * 128
                ]

    for index in range(steps):
        fetch(index).start()
    fetch(0).wait()
    ready_ref[...] = product(0)

    def some(step, carry):
        fetch(step).wait()
        move(step - 1)
        ready_ref[...] = product(step)
        return carry

    lax.fori_loop(1, steps, some, 0)
    move(steps - 1)
    for column in range(spread_ref.shape[0]):
        for block in range(blocks):
            start = block * (panel + 1)
            out_ref[block * panel : (block + 1) * panel, column * 128 : (column + 1) * 128] = (
                spread_ref[column, start : start + panel, :].astype(jnp.bfloat16)
            )


def collect(wanted_ref, parts_ref, rows_ref, gram_ref):
    row_devices, col_devices, _, wide = parts_ref.shape
    width = wide // 2
    groups = []
    for row in range(row_devices):
        total = parts_ref[row, 0].astype(jnp.float32)
        for col in range(1, col_devices):
            total = total + parts_ref[row, col].astype(jnp.float32)
        groups.append(total)
    sample = jnp.concatenate(groups, axis=0).astype(jnp.bfloat16)
    blocks = sample.shape[0]
    wanted = wanted_ref[...]
    rows = wanted.shape[0]
    block = lax.shift_right_logical(wanted, 8)
    inside = lax.bitwise_and(wanted, rows - 1)
    same = block == iota((rows, blocks), 1)
    low = jnp.min(jnp.where(same, inside, rows), axis=0, keepdims=True)
    high = jnp.max(jnp.where(same, inside, -1), axis=0, keepdims=True)
    ordered = jnp.zeros((rows, width), jnp.float32)
    for which, chosen in enumerate((low, high)):
        pick = jnp.where(same & (inside == chosen), 1.0, 0.0).astype(jnp.bfloat16)
        ordered = ordered + jnp.dot(
            pick,
            sample[:, which * width : (which + 1) * width],
            preferred_element_type=jnp.float32,
        )
    ordered = ordered.astype(jnp.bfloat16)
    rows_ref[...] = ordered
    half = width // 2
    down, across = iota((half, half), 0), iota((half, half), 1)
    for unit in range(rows // UNIT):
        piece = ordered[unit * UNIT : (unit + 1) * UNIT]
        left, right = piece[:, :half], piece[:, half:]
        top, side, corner = [
            lax.dot_general(
                one, two, (((0,), (0,)), ((), ())), preferred_element_type=jnp.float32
            )
            for one, two in ((left, left), (right, left), (right, right))
        ]
        diagonal = jnp.sum(jnp.where(across == down, corner, 0.0), axis=0, keepdims=True)
        blocks_of = (
            jnp.where(across <= down, top, corner),
            side,
            jnp.broadcast_to(diagonal, (half, half)),
            jnp.zeros((half, half), jnp.float32),
        )
        for index, values in enumerate(blocks_of):
            gram_ref[pl.ds(unit * 4 + index, half, stride=8), :] = values


def leaf_of_unit(units_ref, unit):
    leaf = jnp.zeros_like(unit)
    end = jnp.int32(0)
    for index in range(units_ref.shape[0]):
        end = end + units_ref[index] + (MINU - 1)
        leaf = leaf + (unit >= end).astype(jnp.int32)
    return leaf


def exact_sum(member, values):
    total = jnp.zeros((member.shape[0], values.shape[1]), jnp.float32)
    for _ in range(3):
        piece = values.astype(jnp.bfloat16)
        values = values - piece.astype(jnp.float32)
        total = total + jnp.dot(member, piece, preferred_element_type=jnp.float32)
    return total


def node_sums(device_ref, units_ref, parts_ref, out_ref, diagonal_ref):
    devices = parts_ref.shape[0] // 8
    lanes = iota((8, devices), 1)
    row_leaf = [leaf_of_unit(units_ref, 2 * lanes + place)[0:1] for place in range(2)]
    row_leaf = jnp.concatenate(row_leaf, axis=1)
    wide = jnp.broadcast_to(row_leaf, (devices, 2 * devices))
    column_leaf = [
        jnp.transpose(wide[:, place * devices : (place + 1) * devices].astype(jnp.float32))
        for place in range(2)
    ]
    column_leaf = jnp.concatenate(column_leaf, axis=0).astype(jnp.int32)
    column_leaf = jnp.concatenate([column_leaf, column_leaf], axis=1)
    row_leaf = jnp.broadcast_to(row_leaf, column_leaf.shape)
    values = []
    for index in range(3):
        pieces = [
            parts_ref[pl.ds(place * 4 + index, devices, stride=8), :] for place in range(2)
        ]
        values.append(jnp.concatenate(pieces, axis=0))
    both = jnp.concatenate(values[:2], axis=1)
    slots = 2 * (LEVELS + 1)
    width = values[0].shape[1]
    for level in range(LEVELS + 1):
        match = lax.shift_right_logical(row_leaf, level) == lax.shift_right_logical(
            column_leaf, level
        )
        total = exact_sum(jnp.where(match, 1.0, 0.0).astype(jnp.bfloat16), both)
        for place in range(2):
            for index in range(2):
                out_ref[pl.ds(index * slots + 2 * level + place, devices, stride=2 * slots), :] = (
                    total[
                        place * devices : (place + 1) * devices,
                        index * width : (index + 1) * width,
                    ]
                )
    slot = iota((slots, 2 * devices), 0)
    level = lax.shift_right_logical(slot, 1)
    own = leaf_of_unit(units_ref, 2 * device_ref[0] + lax.bitwise_and(slot, 1))
    match = lax.shift_right_logical(row_leaf[:slots], level) == lax.shift_right_logical(own, level)
    diagonal_ref[...] = exact_sum(jnp.where(match, 1.0, 0.0).astype(jnp.bfloat16), values[2])


def spread_row(values, row):
    return jnp.broadcast_to(values[row : row + 1], values.shape)


def eliminate(group, base, lane, sub):
    inside = (lane >= base) & (lane < base + 8)
    eye = jnp.where(lane - base == sub, 1.0, 0.0)
    columns = [
        [jnp.broadcast_to(rows[:, base + i : base + i + 1], sub.shape) for i in range(8)]
        for rows in group
    ]
    values = [jnp.where(inside, eye, rows) for rows in group]
    scales = [jnp.zeros(sub.shape, jnp.float32) for _ in group]
    members = range(len(group))
    for i in range(8):
        roots = [lax.rsqrt(spread_row(columns[m][i], i)) for m in members]
        scales = [jnp.where(sub == i, roots[m], scales[m]) for m in members]
        if i < 7:
            below = [
                jnp.where(sub > i, columns[m][i] * (roots[m] * roots[m]), 0.0) for m in members
            ]
            for k in range(i + 1, 8):
                for m in members:
                    columns[m][k] = columns[m][k] - below[m] * spread_row(columns[m][k], i)
            values = [values[m] - below[m] * spread_row(values[m], i) for m in members]
    squares = [scale * scale for scale in scales]
    solved = [values[m] * squares[m] for m in members]
    for i in range(7, 0, -1):
        above = [jnp.where(sub < i, columns[m][i] * squares[m], 0.0) for m in members]
        solved = [solved[m] - above[m] * spread_row(solved[m], i) for m in members]
    return [values[m] * scales[m] for m in members], solved


def invert_factors(work_ref, panel_ref):
    count, size, lanes = work_ref.shape
    deep = panel_ref.shape[1]
    lane = iota((8, lanes), 1)
    sub = iota((8, lanes), 0)
    for start in range(0, size, deep):
        end = start + deep
        for base in range(start, end, 8):
            inside = (lane >= base) & (lane < base + 8)
            in_panel = (lane >= start) & (lane < end)
            done = {}
            for first in range(0, count, TOGETHER):
                batch = range(first, first + TOGETHER)
                pair = eliminate(
                    [work_ref[which, base : base + 8, :] for which in batch], base, lane, sub
                )
                for index, which in enumerate(batch):
                    done[which] = pair[0][index], pair[1][index]
            for which in range(count):
                scaled, solved = done[which]
                lower = lane <= base + sub
                if end < size:
                    panel_ref[which, base - start : base - start + 8, :] = jnp.where(
                        in_panel & (lane > base + sub), 0.0, scaled
                    )
                work_ref[which, base : base + 8, :] = jnp.where(lower, scaled, 0.0)
                for other in range(base + 8, end, 8):
                    rows = work_ref[which, other : other + 8, :]
                    total = jnp.where(inside, 0.0, rows)
                    for i in range(8):
                        column = jnp.broadcast_to(
                            rows[:, base + i : base + i + 1], rows.shape
                        )
                        total = total - column * spread_row(solved, i)
                    work_ref[which, other : other + 8, :] = total
        if end < size:
            wide = iota((deep, lanes), 1)
            rest = iota((size - end, lanes), 1)
            for which in range(count):
                panel = panel_ref[which]
                rows = work_ref[which, end:, :]
                factor = jnp.where((wide >= start) & (wide < end), panel, 0.0)
                part = dot_t(rows, factor)
                work_ref[which, end:, :] = jnp.where(
                    (rest >= start) & (rest < end), 0.0, rows
                ) - jnp.dot(
                    part, panel, precision=HIGHEST, preferred_element_type=jnp.float32
                )


def dot_t(one, two, precision=HIGHEST):
    return lax.dot_general(
        one,
        two,
        (((1,), (1,)), ((), ())),
        precision=precision,
        preferred_element_type=jnp.float32,
    )


def node_bases(
    device_ref,
    units_ref,
    node_ref,
    diagonal_ref,
    rows_ref,
    out_ref,
    work_ref,
    side_ref,
    last_ref,
    panel_ref,
):
    slots = work_ref.shape[0]
    half = work_ref.shape[1]
    stride = 2 * slots
    scales = []
    for slot in range(slots):
        level, unit = slot // 2, 2 * device_ref[0] + slot % 2
        leaf = jnp.int32(0)
        end = jnp.int32(0)
        for index in range(units_ref.shape[0]):
            end = end + units_ref[index] + (MINU - 1)
            leaf = leaf + (unit >= end).astype(jnp.int32)
        node = lax.shift_right_logical(leaf, level)
        count = jnp.int32(0)
        for index in range(units_ref.shape[0]):
            size = units_ref[index] + (MINU - 1)
            count = count + jnp.where(node == index >> level, size, 0)
        size = jnp.full((half, half), count * UNIT, jnp.int32).astype(jnp.float32)
        scales.append(size)
    down, across = iota((half, half), 0), iota((half, half), 1)
    for slot in range(slots):
        corners = node_ref[pl.ds(slot, half, stride=stride), :] / scales[slot]
        turned = jnp.transpose(corners)
        diagonal = jnp.broadcast_to(diagonal_ref[slot : slot + 1, :], (half, half))
        work_ref[slot] = jnp.where(across <= down, corners, turned)
        last_ref[slot] = jnp.where(
            across > down,
            corners,
            jnp.where(across == down, diagonal / scales[slot], turned),
        )
    invert_factors(work_ref, panel_ref)
    for slot in range(slots):
        below = node_ref[pl.ds(slots + slot, half, stride=stride), :] / scales[slot]
        side = dot_t(below, work_ref[slot])
        side_ref[slot] = side
        last_ref[slot] = last_ref[slot] - dot_t(side, side)
    invert_factors(last_ref, panel_ref)
    for slot in range(slots):
        level, unit = slot // 2, slot % 2
        piece = rows_ref[unit * UNIT : (unit + 1) * UNIT, :].astype(jnp.float32)
        first = dot_t(piece[:, :half], work_ref[slot])
        rest = piece[:, half:] - dot_t(first, side_ref[slot])
        second = dot_t(rest, last_ref[slot])
        place = slice(unit * UNIT, (unit + 1) * UNIT)
        out_ref[level, place, :half] = first.astype(jnp.bfloat16)
        out_ref[level, place, half:] = second.astype(jnp.bfloat16)


def shards(kernel, random_cols, tree_perm, leaf_units):
    f32, bf16 = jnp.float32, jnp.bfloat16
    width = random_cols.shape[1]
    half = width // 2
    row_devices, col_devices = lax.axis_size("row"), lax.axis_size("col")
    devices = row_devices * col_devices
    total_rows = tree_perm.shape[0]
    rows_dev = total_rows // devices
    panel = kernel.shape[0] // rows_dev
    slots = 2 * (LEVELS + 1)
    row = lax.axis_index("row")
    device = row * col_devices + lax.axis_index("col")
    vmem = pl.BlockSpec(memory_space=pltpu.VMEM)
    smem = pl.BlockSpec(memory_space=pltpu.SMEM)

    def exchange(values, axes):
        return lax.all_to_all(values, axes, 0, 0, tiled=True)

    partial_w = lax.dot_general(
        kernel, random_cols, (((0,), (0,)), ((), ())), preferred_element_type=f32
    ).astype(bf16)
    chunk = kernel.shape[1] // row_devices
    arrived = exchange(partial_w.reshape(row_devices, chunk, width), "row")
    own_w = jnp.sum(arrived.astype(f32), axis=0).astype(bf16)
    sample_w = exchange(jnp.broadcast_to(own_w[None], (row_devices, chunk, width)), "row")
    sample_w = sample_w.reshape(kernel.shape[1], width)

    tree = tree_perm.reshape(devices, rows_dev)
    hbm = pl.BlockSpec(memory_space=pl.ANY)
    picks = pl.pallas_call(
        choose,
        in_specs=[smem, vmem],
        out_specs=vmem,
        scratch_shapes=[pltpu.VMEM((2, rows_dev, devices), jnp.int32)],
        out_shape=jax.ShapeDtypeStruct((panel, 2 * devices, rows_dev), bf16),
        cost_estimate=pl.CostEstimate(
            flops=1 << 30, bytes_accessed=4 * devices * panel * rows_dev, transcendentals=0
        ),
        name="choose",
    )((row * panel)[None], tree)
    parts = pl.pallas_call(
        second_pass,
        in_specs=[hbm, vmem, vmem],
        out_specs=vmem,
        scratch_shapes=[
            pltpu.VMEM((panel // EACH, EACH * rows_dev, kernel.shape[1]), bf16),
            pltpu.VMEM((EACH * rows_dev, width), bf16),
            pltpu.VMEM((4, devices * (panel + 1), 128), f32),
            pltpu.SemaphoreType.DMA((panel // EACH,)),
        ],
        out_shape=jax.ShapeDtypeStruct((devices * panel, 2 * width), bf16),
        name="second_pass",
    )(kernel, sample_w, picks)
    parts = exchange(parts.reshape(devices, panel, 2 * width), BOTH)
    parts = parts.reshape(row_devices, col_devices, panel, 2 * width)

    wanted = lax.dynamic_slice_in_dim(tree_perm, device * rows_dev, rows_dev)
    wanted = jnp.broadcast_to(wanted[:, None], (rows_dev, devices))
    tree_rows, grams = pl.pallas_call(
        collect,
        in_specs=[vmem, vmem],
        out_specs=[vmem, vmem],
        out_shape=[
            jax.ShapeDtypeStruct((rows_dev, width), bf16),
            jax.ShapeDtypeStruct((devices * 8, half), f32),
        ],
        name="collect",
    )(wanted, parts)

    grams = exchange(grams.reshape(devices, 8, half), BOTH)
    nodes, diagonals = pl.pallas_call(
        node_sums,
        in_specs=[smem, smem, vmem],
        out_specs=[vmem, vmem],
        out_shape=[
            jax.ShapeDtypeStruct((devices * 2 * slots, half), f32),
            jax.ShapeDtypeStruct((slots, half), f32),
        ],
        name="node_sums",
    )(device[None], leaf_units, grams.reshape(devices * 8, half))
    nodes = exchange(nodes.reshape(devices, 2 * slots, half), BOTH)

    return pl.pallas_call(
        node_bases,
        in_specs=[smem, smem, vmem, vmem, vmem],
        out_specs=vmem,
        out_shape=jax.ShapeDtypeStruct((LEVELS + 1, rows_dev, width), bf16),
        scratch_shapes=[pltpu.VMEM((slots, half, half), f32)] * 3
        + [pltpu.VMEM((slots, DEEP, half), f32)],
        name="node_bases",
    )(device[None], leaf_units, nodes.reshape(devices * 2 * slots, half), diagonals, tree_rows)


def solution(mesh):
    return jax.shard_map(
        shards,
        mesh=mesh,
        in_specs=(P("row", "col"), P("row", None), P(), P()),
        out_specs=P(None, ("row", "col"), None),
        check_vma=False,
    )
```

```python
import functools

import jax
import jax.numpy as jnp
from jax import lax
from jax.experimental import pallas as pl
from jax.experimental.pallas import tpu as pltpu
from jax.sharding import PartitionSpec as P

UNIT = 128
MINU = 4
LEVELS = 3
DEEP = 32
TOGETHER = 4
EACH = 2
BOTH = ("row", "col")
HIGHEST = lax.Precision.HIGHEST


def iota(shape, dim):
    return lax.broadcasted_iota(jnp.int32, shape, dim)


def choose(first_ref, tree_ref, out_ref, wanted_ref, turned_ref):
    panel = out_ref.shape[0]
    rows, blocks = turned_ref.shape[1:]
    tree = jnp.transpose(tree_ref[...])
    turned_ref[0] = lax.shift_right_logical(tree, 8)
    turned_ref[1] = lax.bitwise_and(tree, rows - 1)
    own = tree_ref[pl.ds(first_ref[1], 1), :]
    wanted_ref[...] = jnp.transpose(jnp.broadcast_to(own, (blocks, rows)))
    place = iota((rows, blocks), 0)

    def one(step, carry):
        here = turned_ref[0] == first_ref[0] + step
        inner = turned_ref[1]
        low = jnp.min(jnp.where(here, inner, rows), axis=0, keepdims=True)
        high = jnp.max(jnp.where(here, inner, -1), axis=0, keepdims=True)
        for which, chosen in enumerate((low, high)):
            pick = jnp.transpose(jnp.where(place == chosen, 1.0, 0.0))
            out_ref[step, which * blocks : (which + 1) * blocks, :] = pick.astype(jnp.bfloat16)
        return carry

    lax.fori_loop(0, panel, one, 0)


def second_pass(kernel_ref, w_ref, pick_ref, out_ref, held_ref, ready_ref, spread_ref, sems):
    panel, blocks = pick_ref.shape[0], pick_ref.shape[1] // 2
    steps, tall, _ = held_ref.shape
    rows = pick_ref.shape[2]
    each = tall // rows

    def fetch(index):
        return pltpu.make_async_copy(
            kernel_ref.at[pl.ds(index * tall, tall), :], held_ref.at[index], sems.at[index]
        )

    def product(index):
        return jnp.dot(
            held_ref[index], w_ref[...], preferred_element_type=jnp.float32
        ).astype(jnp.bfloat16)

    def move(index):
        for inner in range(each):
            moved = jnp.dot(
                pick_ref[index * each + inner],
                ready_ref[inner * rows : (inner + 1) * rows, :],
                preferred_element_type=jnp.float32,
            )
            for column in range(spread_ref.shape[0]):
                which, half = column // 2, column % 2
                place = pl.ds(index * each + inner, blocks, stride=panel + 1)
                spread_ref[column, place, :] = moved[
                    which * blocks : (which + 1) * blocks, half * 128 : (half + 1) * 128
                ]

    for index in range(steps):
        fetch(index).start()
    fetch(0).wait()
    ready_ref[...] = product(0)

    def some(step, carry):
        fetch(step).wait()
        move(step - 1)
        ready_ref[...] = product(step)
        return carry

    lax.fori_loop(1, steps, some, 0)
    move(steps - 1)
    for column in range(spread_ref.shape[0]):
        for block in range(blocks):
            start = block * (panel + 1)
            out_ref[block * panel : (block + 1) * panel, column * 128 : (column + 1) * 128] = (
                spread_ref[column, start : start + panel, :].astype(jnp.bfloat16)
            )


def collect(wanted_ref, parts_ref, rows_ref, gram_ref):
    row_devices, col_devices, _, wide = parts_ref.shape
    width = wide // 2
    groups = []
    for row in range(row_devices):
        total = parts_ref[row, 0].astype(jnp.float32)
        for col in range(1, col_devices):
            total = total + parts_ref[row, col].astype(jnp.float32)
        groups.append(total)
    sample = jnp.concatenate(groups, axis=0).astype(jnp.bfloat16)
    blocks = sample.shape[0]
    wanted = wanted_ref[...]
    rows = wanted.shape[0]
    block = lax.shift_right_logical(wanted, 8)
    inside = lax.bitwise_and(wanted, rows - 1)
    same = block == iota((rows, blocks), 1)
    low = jnp.min(jnp.where(same, inside, rows), axis=0, keepdims=True)
    high = jnp.max(jnp.where(same, inside, -1), axis=0, keepdims=True)
    ordered = jnp.zeros((rows, width), jnp.float32)
    for which, chosen in enumerate((low, high)):
        pick = jnp.where(same & (inside == chosen), 1.0, 0.0).astype(jnp.bfloat16)
        ordered = ordered + jnp.dot(
            pick,
            sample[:, which * width : (which + 1) * width],
            preferred_element_type=jnp.float32,
        )
    ordered = ordered.astype(jnp.bfloat16)
    rows_ref[...] = ordered
    half = width // 2
    down, across = iota((half, half), 0), iota((half, half), 1)
    for unit in range(rows // UNIT):
        piece = ordered[unit * UNIT : (unit + 1) * UNIT]
        left, right = piece[:, :half], piece[:, half:]
        top, side, corner = [
            lax.dot_general(
                one, two, (((0,), (0,)), ((), ())), preferred_element_type=jnp.float32
            )
            for one, two in ((left, left), (right, left), (right, right))
        ]
        diagonal = jnp.sum(jnp.where(across == down, corner, 0.0), axis=0, keepdims=True)
        blocks_of = (
            jnp.where(across <= down, top, corner),
            side,
            jnp.broadcast_to(diagonal, (half, half)),
            jnp.zeros((half, half), jnp.float32),
        )
        for index, values in enumerate(blocks_of):
            gram_ref[pl.ds(unit * 4 + index, half, stride=8), :] = values


def leaf_of_unit(units_ref, unit):
    leaf = jnp.zeros_like(unit)
    end = jnp.int32(0)
    for index in range(units_ref.shape[0]):
        end = end + units_ref[index] + (MINU - 1)
        leaf = leaf + (unit >= end).astype(jnp.int32)
    return leaf


def exact_sum(member, values):
    total = jnp.zeros((member.shape[0], values.shape[1]), jnp.float32)
    for _ in range(3):
        piece = values.astype(jnp.bfloat16)
        values = values - piece.astype(jnp.float32)
        total = total + jnp.dot(member, piece, preferred_element_type=jnp.float32)
    return total


def node_sums(device_ref, units_ref, parts_ref, out_ref, diagonal_ref):
    devices = parts_ref.shape[0] // 8
    lanes = iota((8, devices), 1)
    row_leaf = [leaf_of_unit(units_ref, 2 * lanes + place)[0:1] for place in range(2)]
    row_leaf = jnp.concatenate(row_leaf, axis=1)
    wide = jnp.broadcast_to(row_leaf, (devices, 2 * devices))
    column_leaf = [
        jnp.transpose(wide[:, place * devices : (place + 1) * devices].astype(jnp.float32))
        for place in range(2)
    ]
    column_leaf = jnp.concatenate(column_leaf, axis=0).astype(jnp.int32)
    column_leaf = jnp.concatenate([column_leaf, column_leaf], axis=1)
    row_leaf = jnp.broadcast_to(row_leaf, column_leaf.shape)
    values = []
    for index in range(3):
        pieces = [
            parts_ref[pl.ds(place * 4 + index, devices, stride=8), :] for place in range(2)
        ]
        values.append(jnp.concatenate(pieces, axis=0))
    both = jnp.concatenate(values[:2], axis=1)
    slots = 2 * (LEVELS + 1)
    width = values[0].shape[1]
    for level in range(LEVELS + 1):
        match = lax.shift_right_logical(row_leaf, level) == lax.shift_right_logical(
            column_leaf, level
        )
        total = exact_sum(jnp.where(match, 1.0, 0.0).astype(jnp.bfloat16), both)
        for place in range(2):
            for index in range(2):
                out_ref[pl.ds(index * slots + 2 * level + place, devices, stride=2 * slots), :] = (
                    total[
                        place * devices : (place + 1) * devices,
                        index * width : (index + 1) * width,
                    ]
                )
    slot = iota((slots, 2 * devices), 0)
    level = lax.shift_right_logical(slot, 1)
    own = leaf_of_unit(units_ref, 2 * device_ref[0] + lax.bitwise_and(slot, 1))
    match = lax.shift_right_logical(row_leaf[:slots], level) == lax.shift_right_logical(own, level)
    diagonal_ref[...] = exact_sum(jnp.where(match, 1.0, 0.0).astype(jnp.bfloat16), values[2])


def spread_row(values, row):
    return jnp.broadcast_to(values[row : row + 1], values.shape)


def eliminate(group, base, lane, sub):
    inside = (lane >= base) & (lane < base + 8)
    eye = jnp.where(lane - base == sub, 1.0, 0.0)
    columns = [
        [jnp.broadcast_to(rows[:, base + i : base + i + 1], sub.shape) for i in range(8)]
        for rows in group
    ]
    values = [jnp.where(inside, eye, rows) for rows in group]
    scales = [jnp.zeros(sub.shape, jnp.float32) for _ in group]
    members = range(len(group))
    for i in range(8):
        roots = [lax.rsqrt(spread_row(columns[m][i], i)) for m in members]
        scales = [jnp.where(sub == i, roots[m], scales[m]) for m in members]
        if i < 7:
            below = [
                jnp.where(sub > i, columns[m][i] * (roots[m] * roots[m]), 0.0) for m in members
            ]
            for k in range(i + 1, 8):
                for m in members:
                    columns[m][k] = columns[m][k] - below[m] * spread_row(columns[m][k], i)
            values = [values[m] - below[m] * spread_row(values[m], i) for m in members]
    squares = [scale * scale for scale in scales]
    solved = [values[m] * squares[m] for m in members]
    for i in range(7, 0, -1):
        above = [jnp.where(sub < i, columns[m][i] * squares[m], 0.0) for m in members]
        solved = [solved[m] - above[m] * spread_row(solved[m], i) for m in members]
    return [values[m] * scales[m] for m in members], solved


def invert_factors(work_ref, panel_ref):
    count, size, lanes = work_ref.shape
    deep = panel_ref.shape[1]
    lane = iota((8, lanes), 1)
    sub = iota((8, lanes), 0)
    for start in range(0, size, deep):
        end = start + deep
        for base in range(start, end, 8):
            inside = (lane >= base) & (lane < base + 8)
            in_panel = (lane >= start) & (lane < end)
            done = {}
            for first in range(0, count, TOGETHER):
                batch = range(first, first + TOGETHER)
                pair = eliminate(
                    [work_ref[which, base : base + 8, :] for which in batch], base, lane, sub
                )
                for index, which in enumerate(batch):
                    done[which] = pair[0][index], pair[1][index]
            for which in range(count):
                scaled, solved = done[which]
                lower = lane <= base + sub
                if end < size:
                    panel_ref[which, base - start : base - start + 8, :] = jnp.where(
                        in_panel & (lane > base + sub), 0.0, scaled
                    )
                work_ref[which, base : base + 8, :] = jnp.where(lower, scaled, 0.0)
                for other in range(base + 8, end, 8):
                    rows = work_ref[which, other : other + 8, :]
                    total = jnp.where(inside, 0.0, rows)
                    for i in range(8):
                        column = jnp.broadcast_to(
                            rows[:, base + i : base + i + 1], rows.shape
                        )
                        total = total - column * spread_row(solved, i)
                    work_ref[which, other : other + 8, :] = total
        if end < size:
            wide = iota((deep, lanes), 1)
            rest = iota((size - end, lanes), 1)
            for which in range(count):
                panel = panel_ref[which]
                rows = work_ref[which, end:, :]
                factor = jnp.where((wide >= start) & (wide < end), panel, 0.0)
                part = dot_t(rows, factor)
                work_ref[which, end:, :] = jnp.where(
                    (rest >= start) & (rest < end), 0.0, rows
                ) - jnp.dot(
                    part, panel, precision=HIGHEST, preferred_element_type=jnp.float32
                )


def dot_t(one, two, precision=HIGHEST):
    return lax.dot_general(
        one,
        two,
        (((1,), (1,)), ((), ())),
        precision=precision,
        preferred_element_type=jnp.float32,
    )


def node_bases(
    device_ref,
    units_ref,
    node_ref,
    diagonal_ref,
    rows_ref,
    out_ref,
    work_ref,
    side_ref,
    last_ref,
    panel_ref,
):
    slots = work_ref.shape[0]
    half = work_ref.shape[1]
    stride = 2 * slots
    scales = []
    for slot in range(slots):
        level, unit = slot // 2, 2 * device_ref[0] + slot % 2
        leaf = jnp.int32(0)
        end = jnp.int32(0)
        for index in range(units_ref.shape[0]):
            end = end + units_ref[index] + (MINU - 1)
            leaf = leaf + (unit >= end).astype(jnp.int32)
        node = lax.shift_right_logical(leaf, level)
        count = jnp.int32(0)
        for index in range(units_ref.shape[0]):
            size = units_ref[index] + (MINU - 1)
            count = count + jnp.where(node == index >> level, size, 0)
        size = jnp.full((half, half), count * UNIT, jnp.int32).astype(jnp.float32)
        scales.append(size)
    down, across = iota((half, half), 0), iota((half, half), 1)
    for slot in range(slots):
        corners = node_ref[pl.ds(slot, half, stride=stride), :] / scales[slot]
        turned = jnp.transpose(corners)
        diagonal = jnp.broadcast_to(diagonal_ref[slot : slot + 1, :], (half, half))
        work_ref[slot] = jnp.where(across <= down, corners, turned)
        last_ref[slot] = jnp.where(
            across > down,
            corners,
            jnp.where(across == down, diagonal / scales[slot], turned),
        )
    invert_factors(work_ref, panel_ref)
    for slot in range(slots):
        below = node_ref[pl.ds(slots + slot, half, stride=stride), :] / scales[slot]
        side = dot_t(below, work_ref[slot])
        side_ref[slot] = side
        last_ref[slot] = last_ref[slot] - dot_t(side, side)
    invert_factors(last_ref, panel_ref)
    for slot in range(slots):
        level, unit = slot // 2, slot % 2
        piece = rows_ref[unit * UNIT : (unit + 1) * UNIT, :].astype(jnp.float32)
        first = dot_t(piece[:, :half], work_ref[slot])
        rest = piece[:, half:] - dot_t(first, side_ref[slot])
        second = dot_t(rest, last_ref[slot])
        place = slice(unit * UNIT, (unit + 1) * UNIT)
        out_ref[level, place, :half] = first.astype(jnp.bfloat16)
        out_ref[level, place, half:] = second.astype(jnp.bfloat16)


def shards(kernel, random_cols, tree_perm, leaf_units):
    f32, bf16 = jnp.float32, jnp.bfloat16
    width = random_cols.shape[1]
    half = width // 2
    row_devices, col_devices = lax.axis_size("row"), lax.axis_size("col")
    devices = row_devices * col_devices
    total_rows = tree_perm.shape[0]
    rows_dev = total_rows // devices
    panel = kernel.shape[0] // rows_dev
    slots = 2 * (LEVELS + 1)
    row = lax.axis_index("row")
    device = row * col_devices + lax.axis_index("col")
    vmem = pl.BlockSpec(memory_space=pltpu.VMEM)
    smem = pl.BlockSpec(memory_space=pltpu.SMEM)

    def near(values):
        return pltpu.with_memory_space_constraint(values, pltpu.VMEM)

    def exchange(values, axes):
        return lax.all_to_all(values, axes, 0, 0, tiled=True)

    partial_w = lax.dot_general(
        kernel, random_cols, (((0,), (0,)), ((), ())), preferred_element_type=f32
    ).astype(bf16)
    chunk = kernel.shape[1] // row_devices
    arrived = exchange(partial_w.reshape(row_devices, chunk, width), "row")
    own_w = jnp.sum(arrived.astype(f32), axis=0).astype(bf16)
    sample_w = exchange(jnp.broadcast_to(own_w[None], (row_devices, chunk, width)), "row")
    sample_w = sample_w.reshape(kernel.shape[1], width)

    tree = tree_perm.reshape(devices, rows_dev)
    hbm = pl.BlockSpec(memory_space=pl.ANY)
    picks, wanted = pl.pallas_call(
        choose,
        in_specs=[smem, vmem],
        out_specs=[vmem, vmem],
        scratch_shapes=[pltpu.VMEM((2, rows_dev, devices), jnp.int32)],
        out_shape=[
            jax.ShapeDtypeStruct((panel, 2 * devices, rows_dev), bf16),
            jax.ShapeDtypeStruct((rows_dev, devices), jnp.int32),
        ],
        cost_estimate=pl.CostEstimate(
            flops=1 << 30, bytes_accessed=4 * devices * panel * rows_dev, transcendentals=0
        ),
        name="choose",
    )(jnp.stack([row * panel, device]), tree)
    parts = pl.pallas_call(
        second_pass,
        in_specs=[hbm, vmem, vmem],
        out_specs=vmem,
        scratch_shapes=[
            pltpu.VMEM((panel // EACH, EACH * rows_dev, kernel.shape[1]), bf16),
            pltpu.VMEM((EACH * rows_dev, width), bf16),
            pltpu.VMEM((4, devices * (panel + 1), 128), f32),
            pltpu.SemaphoreType.DMA((panel // EACH,)),
        ],
        out_shape=jax.ShapeDtypeStruct((devices * panel, 2 * width), bf16),
        name="second_pass",
    )(kernel, near(sample_w), picks)
    parts = exchange(parts.reshape(devices, panel, 2 * width), BOTH)
    parts = parts.reshape(row_devices, col_devices, panel, 2 * width)

    tree_rows, grams = pl.pallas_call(
        collect,
        in_specs=[vmem, vmem],
        out_specs=[vmem, vmem],
        out_shape=[
            jax.ShapeDtypeStruct((rows_dev, width), bf16),
            pltpu.VMEM((devices * 8, half), f32),
        ],
        name="collect",
    )(wanted, near(parts))

    grams = exchange(grams.reshape(devices, 8, half), BOTH)
    nodes, diagonals = pl.pallas_call(
        node_sums,
        in_specs=[smem, smem, vmem],
        out_specs=[vmem, vmem],
        out_shape=[
            pltpu.VMEM((devices * 2 * slots, half), f32),
            jax.ShapeDtypeStruct((slots, half), f32),
        ],
        name="node_sums",
    )(device[None], leaf_units, near(grams.reshape(devices * 8, half)))
    nodes = exchange(nodes.reshape(devices, 2 * slots, half), BOTH)

    return pl.pallas_call(
        node_bases,
        in_specs=[smem, smem, vmem, vmem, vmem],
        out_specs=vmem,
        out_shape=jax.ShapeDtypeStruct((LEVELS + 1, rows_dev, width), bf16),
        scratch_shapes=[pltpu.VMEM((slots, half, half), f32)] * 3
        + [pltpu.VMEM((slots, DEEP, half), f32)],
        name="node_bases",
    )(device[None], leaf_units, near(nodes.reshape(devices * 2 * slots, half)), diagonals, tree_rows)


def solution(mesh):
    return jax.shard_map(
        shards,
        mesh=mesh,
        in_specs=(P("row", "col"), P("row", None), P(), P()),
        out_specs=P(None, ("row", "col"), None),
        check_vma=False,
    )
```

```python
import functools

import jax
import jax.numpy as jnp
from jax import lax
from jax.experimental import pallas as pl
from jax.experimental.pallas import tpu as pltpu
from jax.sharding import PartitionSpec as P

UNIT = 128
MINU = 4
LEVELS = 3
DEEP = 32
TOGETHER = 4
EACH = 2
BOTH = ("row", "col")
HIGHEST = lax.Precision.HIGHEST


def iota(shape, dim):
    return lax.broadcasted_iota(jnp.int32, shape, dim)


def choose(first_ref, tree_ref, out_ref, wanted_ref, turned_ref):
    panel = out_ref.shape[0]
    rows, blocks = turned_ref.shape[1:]
    tree = jnp.transpose(tree_ref[...])
    turned_ref[0] = lax.shift_right_logical(tree, 8)
    turned_ref[1] = lax.bitwise_and(tree, rows - 1)
    own = tree_ref[pl.ds(first_ref[1], 1), :]
    wanted_ref[...] = jnp.transpose(jnp.broadcast_to(own, (blocks, rows)))
    place = iota((rows, blocks), 0)

    def one(step, carry):
        here = turned_ref[0] == first_ref[0] + step
        inner = turned_ref[1]
        low = jnp.min(jnp.where(here, inner, rows), axis=0, keepdims=True)
        high = jnp.max(jnp.where(here, inner, -1), axis=0, keepdims=True)
        for which, chosen in enumerate((low, high)):
            pick = jnp.transpose(jnp.where(place == chosen, 1.0, 0.0))
            out_ref[step, which * blocks : (which + 1) * blocks, :] = pick.astype(jnp.bfloat16)
        return carry

    lax.fori_loop(0, panel, one, 0)


def second_pass(kernel_ref, w_ref, pick_ref, out_ref, held_ref, ready_ref, spread_ref, sems):
    panel, blocks = pick_ref.shape[0], pick_ref.shape[1] // 2
    steps, tall, _ = held_ref.shape
    rows = pick_ref.shape[2]
    each = tall // rows

    def fetch(index):
        return pltpu.make_async_copy(
            kernel_ref.at[pl.ds(index * tall, tall), :], held_ref.at[index], sems.at[index]
        )

    def product(index):
        return jnp.dot(
            held_ref[index], w_ref[...], preferred_element_type=jnp.float32
        ).astype(jnp.bfloat16)

    def move(index):
        for inner in range(each):
            moved = jnp.dot(
                pick_ref[index * each + inner],
                ready_ref[inner * rows : (inner + 1) * rows, :],
                preferred_element_type=jnp.float32,
            )
            for column in range(spread_ref.shape[0]):
                which, half = column // 2, column % 2
                place = pl.ds(index * each + inner, blocks, stride=panel + 1)
                spread_ref[column, place, :] = moved[
                    which * blocks : (which + 1) * blocks, half * 128 : (half + 1) * 128
                ]

    for index in range(steps):
        fetch(index).start()
    fetch(0).wait()
    ready_ref[...] = product(0)

    def some(step, carry):
        fetch(step).wait()
        move(step - 1)
        ready_ref[...] = product(step)
        return carry

    lax.fori_loop(1, steps, some, 0)
    move(steps - 1)
    for column in range(spread_ref.shape[0]):
        for block in range(blocks):
            start = block * (panel + 1)
            out_ref[block * panel : (block + 1) * panel, column * 128 : (column + 1) * 128] = (
                spread_ref[column, start : start + panel, :].astype(jnp.bfloat16)
            )


def collect(wanted_ref, parts_ref, rows_ref, gram_ref):
    row_devices, col_devices, _, wide = parts_ref.shape
    width = wide // 2
    groups = []
    for row in range(row_devices):
        total = parts_ref[row, 0].astype(jnp.float32)
        for col in range(1, col_devices):
            total = total + parts_ref[row, col].astype(jnp.float32)
        groups.append(total)
    sample = jnp.concatenate(groups, axis=0).astype(jnp.bfloat16)
    blocks = sample.shape[0]
    wanted = wanted_ref[...]
    rows = wanted.shape[0]
    block = lax.shift_right_logical(wanted, 8)
    inside = lax.bitwise_and(wanted, rows - 1)
    same = block == iota((rows, blocks), 1)
    low = jnp.min(jnp.where(same, inside, rows), axis=0, keepdims=True)
    high = jnp.max(jnp.where(same, inside, -1), axis=0, keepdims=True)
    ordered = jnp.zeros((rows, width), jnp.float32)
    for which, chosen in enumerate((low, high)):
        pick = jnp.where(same & (inside == chosen), 1.0, 0.0).astype(jnp.bfloat16)
        ordered = ordered + jnp.dot(
            pick,
            sample[:, which * width : (which + 1) * width],
            preferred_element_type=jnp.float32,
        )
    ordered = ordered.astype(jnp.bfloat16)
    rows_ref[...] = ordered
    half = width // 2
    down, across = iota((half, half), 0), iota((half, half), 1)
    for unit in range(rows // UNIT):
        piece = ordered[unit * UNIT : (unit + 1) * UNIT]
        left, right = piece[:, :half], piece[:, half:]
        top, side, corner = [
            lax.dot_general(
                one, two, (((0,), (0,)), ((), ())), preferred_element_type=jnp.float32
            )
            for one, two in ((left, left), (right, left), (right, right))
        ]
        diagonal = jnp.sum(jnp.where(across == down, corner, 0.0), axis=0, keepdims=True)
        blocks_of = (
            jnp.where(across <= down, top, corner),
            side,
            jnp.broadcast_to(diagonal, (half, half)),
            jnp.zeros((half, half), jnp.float32),
        )
        for index, values in enumerate(blocks_of):
            gram_ref[pl.ds(unit * 4 + index, half, stride=8), :] = values


def leaf_of_unit(units_ref, unit):
    leaf = jnp.zeros_like(unit)
    end = jnp.int32(0)
    for index in range(units_ref.shape[0]):
        end = end + units_ref[index] + (MINU - 1)
        leaf = leaf + (unit >= end).astype(jnp.int32)
    return leaf


def exact_sum(member, values):
    total = jnp.zeros((member.shape[0], values.shape[1]), jnp.float32)
    for _ in range(3):
        piece = values.astype(jnp.bfloat16)
        values = values - piece.astype(jnp.float32)
        total = total + jnp.dot(member, piece, preferred_element_type=jnp.float32)
    return total


def node_sums(device_ref, units_ref, parts_ref, out_ref, diagonal_ref):
    devices = parts_ref.shape[0] // 8
    lanes = iota((8, devices), 1)
    row_leaf = [leaf_of_unit(units_ref, 2 * lanes + place)[0:1] for place in range(2)]
    row_leaf = jnp.concatenate(row_leaf, axis=1)
    wide = jnp.broadcast_to(row_leaf, (devices, 2 * devices))
    column_leaf = [
        jnp.transpose(wide[:, place * devices : (place + 1) * devices].astype(jnp.float32))
        for place in range(2)
    ]
    column_leaf = jnp.concatenate(column_leaf, axis=0).astype(jnp.int32)
    column_leaf = jnp.concatenate([column_leaf, column_leaf], axis=1)
    row_leaf = jnp.broadcast_to(row_leaf, column_leaf.shape)
    values = []
    for index in range(3):
        pieces = [
            parts_ref[pl.ds(place * 4 + index, devices, stride=8), :] for place in range(2)
        ]
        values.append(jnp.concatenate(pieces, axis=0))
    both = jnp.concatenate(values[:2], axis=1)
    slots = 2 * (LEVELS + 1)
    width = values[0].shape[1]
    for level in range(LEVELS + 1):
        match = lax.shift_right_logical(row_leaf, level) == lax.shift_right_logical(
            column_leaf, level
        )
        total = exact_sum(jnp.where(match, 1.0, 0.0).astype(jnp.bfloat16), both)
        for place in range(2):
            for index in range(2):
                out_ref[pl.ds(index * slots + 2 * level + place, devices, stride=2 * slots), :] = (
                    total[
                        place * devices : (place + 1) * devices,
                        index * width : (index + 1) * width,
                    ]
                )
    slot = iota((slots, 2 * devices), 0)
    level = lax.shift_right_logical(slot, 1)
    own = leaf_of_unit(units_ref, 2 * device_ref[0] + lax.bitwise_and(slot, 1))
    match = lax.shift_right_logical(row_leaf[:slots], level) == lax.shift_right_logical(own, level)
    diagonal_ref[...] = exact_sum(jnp.where(match, 1.0, 0.0).astype(jnp.bfloat16), values[2])


def spread_row(values, row):
    return jnp.broadcast_to(values[row : row + 1], values.shape)


def eliminate(group, base, lane, sub):
    inside = (lane >= base) & (lane < base + 8)
    eye = jnp.where(lane - base == sub, 1.0, 0.0)
    columns = [
        [jnp.broadcast_to(rows[:, base + i : base + i + 1], sub.shape) for i in range(8)]
        for rows in group
    ]
    values = [jnp.where(inside, eye, rows) for rows in group]
    scales = [jnp.zeros(sub.shape, jnp.float32) for _ in group]
    members = range(len(group))
    for i in range(8):
        roots = [lax.rsqrt(spread_row(columns[m][i], i)) for m in members]
        scales = [jnp.where(sub == i, roots[m], scales[m]) for m in members]
        if i < 7:
            below = [
                jnp.where(sub > i, columns[m][i] * (roots[m] * roots[m]), 0.0) for m in members
            ]
            for k in range(i + 1, 8):
                for m in members:
                    columns[m][k] = columns[m][k] - below[m] * spread_row(columns[m][k], i)
            values = [values[m] - below[m] * spread_row(values[m], i) for m in members]
    squares = [scale * scale for scale in scales]
    solved = [values[m] * squares[m] for m in members]
    for i in range(7, 0, -1):
        above = [jnp.where(sub < i, columns[m][i] * squares[m], 0.0) for m in members]
        solved = [solved[m] - above[m] * spread_row(solved[m], i) for m in members]
    return [values[m] * scales[m] for m in members], solved


def invert_factors(work_ref, panel_ref):
    count, size, lanes = work_ref.shape
    deep = panel_ref.shape[1]
    lane = iota((8, lanes), 1)
    sub = iota((8, lanes), 0)
    for start in range(0, size, deep):
        end = start + deep
        for base in range(start, end, 8):
            inside = (lane >= base) & (lane < base + 8)
            in_panel = (lane >= start) & (lane < end)
            done = {}
            for first in range(0, count, TOGETHER):
                batch = range(first, first + TOGETHER)
                pair = eliminate(
                    [work_ref[which, base : base + 8, :] for which in batch], base, lane, sub
                )
                for index, which in enumerate(batch):
                    done[which] = pair[0][index], pair[1][index]
            for which in range(count):
                scaled, solved = done[which]
                lower = lane <= base + sub
                if end < size:
                    panel_ref[which, base - start : base - start + 8, :] = jnp.where(
                        in_panel & (lane > base + sub), 0.0, scaled
                    )
                work_ref[which, base : base + 8, :] = jnp.where(lower, scaled, 0.0)
                for other in range(base + 8, end, 8):
                    rows = work_ref[which, other : other + 8, :]
                    total = jnp.where(inside, 0.0, rows)
                    for i in range(8):
                        column = jnp.broadcast_to(
                            rows[:, base + i : base + i + 1], rows.shape
                        )
                        total = total - column * spread_row(solved, i)
                    work_ref[which, other : other + 8, :] = total
        if end < size:
            wide = iota((deep, lanes), 1)
            rest = iota((size - end, lanes), 1)
            for which in range(count):
                panel = panel_ref[which]
                rows = work_ref[which, end:, :]
                factor = jnp.where((wide >= start) & (wide < end), panel, 0.0)
                part = dot_t(rows, factor)
                work_ref[which, end:, :] = jnp.where(
                    (rest >= start) & (rest < end), 0.0, rows
                ) - jnp.dot(
                    part, panel, precision=HIGHEST, preferred_element_type=jnp.float32
                )


def dot_t(one, two, precision=HIGHEST):
    return lax.dot_general(
        one,
        two,
        (((1,), (1,)), ((), ())),
        precision=precision,
        preferred_element_type=jnp.float32,
    )


def node_bases(
    device_ref,
    units_ref,
    node_ref,
    diagonal_ref,
    rows_ref,
    out_ref,
    work_ref,
    side_ref,
    last_ref,
    panel_ref,
):
    slots = work_ref.shape[0]
    half = work_ref.shape[1]
    stride = 2 * slots
    scales = []
    for slot in range(slots):
        level, unit = slot // 2, 2 * device_ref[0] + slot % 2
        leaf = jnp.int32(0)
        end = jnp.int32(0)
        for index in range(units_ref.shape[0]):
            end = end + units_ref[index] + (MINU - 1)
            leaf = leaf + (unit >= end).astype(jnp.int32)
        node = lax.shift_right_logical(leaf, level)
        count = jnp.int32(0)
        for index in range(units_ref.shape[0]):
            size = units_ref[index] + (MINU - 1)
            count = count + jnp.where(node == index >> level, size, 0)
        size = jnp.full((half, half), count * UNIT, jnp.int32).astype(jnp.float32)
        scales.append(size)
    down, across = iota((half, half), 0), iota((half, half), 1)
    for slot in range(slots):
        corners = node_ref[pl.ds(slot, half, stride=stride), :] / scales[slot]
        turned = jnp.transpose(corners)
        diagonal = jnp.broadcast_to(diagonal_ref[slot : slot + 1, :], (half, half))
        work_ref[slot] = jnp.where(across <= down, corners, turned)
        last_ref[slot] = jnp.where(
            across > down,
            corners,
            jnp.where(across == down, diagonal / scales[slot], turned),
        )
    invert_factors(work_ref, panel_ref)
    for slot in range(slots):
        below = node_ref[pl.ds(slots + slot, half, stride=stride), :] / scales[slot]
        side = dot_t(below, work_ref[slot])
        side_ref[slot] = side
        last_ref[slot] = last_ref[slot] - dot_t(side, side)
    invert_factors(last_ref, panel_ref)
    for slot in range(slots):
        level, unit = slot // 2, slot % 2
        piece = rows_ref[unit * UNIT : (unit + 1) * UNIT, :].astype(jnp.float32)
        first = dot_t(piece[:, :half], work_ref[slot])
        rest = piece[:, half:] - dot_t(first, side_ref[slot])
        second = dot_t(rest, last_ref[slot])
        place = slice(unit * UNIT, (unit + 1) * UNIT)
        out_ref[level, place, :half] = first.astype(jnp.bfloat16)
        out_ref[level, place, half:] = second.astype(jnp.bfloat16)


def shards(kernel, random_cols, tree_perm, leaf_units):
    f32, bf16 = jnp.float32, jnp.bfloat16
    width = random_cols.shape[1]
    half = width // 2
    row_devices, col_devices = lax.axis_size("row"), lax.axis_size("col")
    devices = row_devices * col_devices
    total_rows = tree_perm.shape[0]
    rows_dev = total_rows // devices
    panel = kernel.shape[0] // rows_dev
    slots = 2 * (LEVELS + 1)
    row = lax.axis_index("row")
    device = row * col_devices + lax.axis_index("col")
    vmem = pl.BlockSpec(memory_space=pltpu.VMEM)
    smem = pl.BlockSpec(memory_space=pltpu.SMEM)

    def near(values):
        return pltpu.with_memory_space_constraint(values, pltpu.VMEM)

    def exchange(values, axes):
        return lax.all_to_all(values, axes, 0, 0, tiled=True)

    partial_w = lax.dot_general(
        kernel, random_cols, (((0,), (0,)), ((), ())), preferred_element_type=f32
    ).astype(bf16)
    chunk = kernel.shape[1] // row_devices
    arrived = exchange(partial_w.reshape(row_devices, chunk, width), "row")
    own_w = jnp.sum(arrived.astype(f32), axis=0).astype(bf16)
    sample_w = exchange(jnp.broadcast_to(own_w[None], (row_devices, chunk, width)), "row")
    sample_w = sample_w.reshape(kernel.shape[1], width)

    tree = tree_perm.reshape(devices, rows_dev)
    hbm = pl.BlockSpec(memory_space=pl.ANY)
    picks, wanted = pl.pallas_call(
        choose,
        in_specs=[smem, vmem],
        out_specs=[vmem, vmem],
        scratch_shapes=[pltpu.VMEM((2, rows_dev, devices), jnp.int32)],
        out_shape=[
            jax.ShapeDtypeStruct((panel, 2 * devices, rows_dev), bf16),
            jax.ShapeDtypeStruct((rows_dev, devices), jnp.int32),
        ],
        cost_estimate=pl.CostEstimate(
            flops=1 << 30, bytes_accessed=4 * devices * panel * rows_dev, transcendentals=0
        ),
        name="choose",
    )(jnp.stack([row * panel, device]), tree)
    parts = pl.pallas_call(
        second_pass,
        in_specs=[hbm, vmem, vmem],
        out_specs=vmem,
        scratch_shapes=[
            pltpu.VMEM((panel // EACH, EACH * rows_dev, kernel.shape[1]), bf16),
            pltpu.VMEM((EACH * rows_dev, width), bf16),
            pltpu.VMEM((4, devices * (panel + 1), 128), f32),
            pltpu.SemaphoreType.DMA((panel // EACH,)),
        ],
        out_shape=jax.ShapeDtypeStruct((devices * panel, 2 * width), bf16),
        name="second_pass",
    )(kernel, near(sample_w), picks)
    parts = parts * (leaf_units[0] > 0).astype(bf16)
    parts = exchange(parts.reshape(devices, panel, 2 * width), BOTH)
    parts = parts.reshape(row_devices, col_devices, panel, 2 * width)

    tree_rows, grams = pl.pallas_call(
        collect,
        in_specs=[vmem, vmem],
        out_specs=[vmem, vmem],
        out_shape=[
            jax.ShapeDtypeStruct((rows_dev, width), bf16),
            pltpu.VMEM((devices * 8, half), f32),
        ],
        name="collect",
    )(wanted, near(parts))

    grams = exchange(grams.reshape(devices, 8, half), BOTH)
    nodes, diagonals = pl.pallas_call(
        node_sums,
        in_specs=[smem, smem, vmem],
        out_specs=[vmem, vmem],
        out_shape=[
            pltpu.VMEM((devices * 2 * slots, half), f32),
            jax.ShapeDtypeStruct((slots, half), f32),
        ],
        name="node_sums",
    )(device[None], leaf_units, near(grams.reshape(devices * 8, half)))
    nodes = exchange(nodes.reshape(devices, 2 * slots, half), BOTH)

    return pl.pallas_call(
        node_bases,
        in_specs=[smem, smem, vmem, vmem, vmem],
        out_specs=vmem,
        out_shape=jax.ShapeDtypeStruct((LEVELS + 1, rows_dev, width), bf16),
        scratch_shapes=[pltpu.VMEM((slots, half, half), f32)] * 3
        + [pltpu.VMEM((slots, DEEP, half), f32)],
        name="node_bases",
    )(device[None], leaf_units, near(nodes.reshape(devices * 2 * slots, half)), diagonals, tree_rows)


def solution(mesh):
    return jax.shard_map(
        shards,
        mesh=mesh,
        in_specs=(P("row", "col"), P("row", None), P(), P()),
        out_specs=P(None, ("row", "col"), None),
        check_vma=False,
    )
```
